32 devices in a mesh: grp: 2 (over y), mesh: 16 (over z, x, core).
Axes of the slice: x: 2, y: 2, z: 4, core: 2. Of those that a mesh axis runs over, the one named last changes fastest.
Arguments:
- state: float32 [2, 5, 256, 4096], P('grp', None, 'mesh'), may hold values from -6 to 6
- burn_rate: float32 [2, 256, 4096], P('grp', 'mesh'), may hold values from 0.1 to 1
- face_map: int32 [2, 16, 1024], P('grp', 'mesh'), may hold values from 0 to 1023, as said below
Outputs:
- new_state: float32 [2, 5, 256, 4096], P('grp', None, 'mesh')
- head: float32 [2, 256, 4096], P('grp', 'mesh')
The draws below stay inside these ranges and needn't reach their ends.
Inputs may be any that keep to these rules, and one draw needn't show every extreme that they name: `face_map`: entry k * 64 + j of a mesh names the cell of its partner's interface plane that feeds its ghost cell (k, j).
All inputs are finite; a program needn't handle non-finite values.
Results may differ from the reference program's by a relative error of at most 0.00025.
Values sent between devices are 32-bit elements; how exact they have to be, the bound alone decides.
No kernel may reach another device: no remote copies, remote signals or barrier semaphores. Data moves between devices by JAX's collectives and lax.ppermute only.
A program may use at most 64 MiB of HBM per device.

```python
import math
import jax
import jax.numpy as jnp
from jax import lax

NX = 64
NY = 64
CZ = 16
FIELDS = 5
SECTIONS = 2
ITERS = 3
NZ = 256
N_MESH = 16


def draw_face_map(key, part):
    offset_z = jax.random.randint(jax.random.fold_in(key, 101), (N_MESH, 1), 0, CZ - CZ // 4 + 1)
    offset_y = jax.random.randint(jax.random.fold_in(key, 102), (N_MESH, 1), 0, NY - NY // 4 + 1)
    cells = jnp.arange(CZ * NY, dtype=jnp.int32)[None, :]
    row_z = cells // NY
    row_y = cells % NY
    fine_rows = (offset_z + row_z // 4) * NY + (offset_y + row_y // 4)
    jitter_z = jax.random.randint(jax.random.fold_in(key, 103), (N_MESH, CZ * NY), 0, 4)
    jitter_y = jax.random.randint(jax.random.fold_in(key, 104), (N_MESH, CZ * NY), 0, 4)
    coarse_z = jnp.clip(4 * (row_z - offset_z) + jitter_z, 0, CZ - 1)
    coarse_y = jnp.clip(4 * (row_y - offset_y) + jitter_y, 0, NY - 1)
    coarse_rows = coarse_z * NY + coarse_y
    return jnp.stack([fine_rows, coarse_rows]).astype(jnp.int32)


def level_of(rng, extent, pieces, smallest, high):
    def one(axis_at, parts):
        heights = jax.random.uniform(jax.random.fold_in(jax.random.fold_in(rng, 6), axis_at), (parts,), jnp.float32, smallest / len(pieces), high / len(pieces))
        return jnp.repeat(jnp.exp(heights), extent[axis_at] // parts).reshape((-1,) + (1,) * (len(extent) - axis_at - 1))

    gain = one(*pieces[0])
    for cut in pieces[1:]:
        gain = gain * one(*cut)
    return gain


def gaussian(stream_key, shape, spread, reach, cuts=(), kind=jnp.bfloat16):
    factor_of = level_of(stream_key, shape, cuts, -0.22, 0.18) if cuts else 1.0
    values = jax.random.normal(stream_key, shape, jnp.float32) * spread * factor_of
    return jnp.minimum(jnp.maximum(values, -reach), reach).astype(kind)


def setup_inputs(seed: int = 0) -> dict:
    seeds = jax.random.split(jax.random.key(seed), 4)
    state = gaussian(seeds[0], (2, FIELDS, NZ, NX * NY), 1.0, 6.0, ((0, 2), (2, 16)), jnp.float32)
    burn_rate = jnp.clip(jnp.exp(math.log(1.0) - 2.3025851 * jax.random.uniform(seeds[1], (2, NZ, NX * NY), jnp.float32) ** level_of(seeds[1], (2, NZ, NX * NY), ((0, 2), (1, 16)), -0.2, 0.2)), 0.1, 1.0)
    face_map = draw_face_map(jax.random.fold_in(seeds[3], 71), 0)
    return dict(state=state, burn_rate=burn_rate, face_map=face_map)


COURANT = 0.1
DIFFUSION = 0.05
STOICHIOMETRY = 2.0
EXPANSION = 1.0

def sine_table(length):
    places = jnp.arange(length, dtype=jnp.float32) + 1.0
    angles = jnp.pi * places[:, None] * places[None, :] / (length + 1)
    return jnp.sin(angles) * jnp.sqrt(2.0 / (length + 1))

def mode_values(length):
    places = jnp.arange(length, dtype=jnp.float32) + 1.0
    return 2.0 - 2.0 * jnp.cos(jnp.pi * places / (length + 1))

def poisson_solve(source):
    table_z = sine_table(source.shape[1]).astype(source.dtype)
    table_x = sine_table(source.shape[2]).astype(source.dtype)
    table_y = sine_table(source.shape[3]).astype(source.dtype)
    precise = lax.Precision.HIGHEST
    spectral = jnp.einsum('ck,mkij->mcij', table_z, source, precision=precise)
    spectral = jnp.einsum('ai,mcij->mcaj', table_x, spectral, precision=precise)
    spectral = jnp.einsum('mcaj,jb->mcab', spectral, table_y, precision=precise)
    modes = (mode_values(source.shape[1])[:, None, None] + mode_values(source.shape[2])[None, :, None] + mode_values(source.shape[3])[None, None, :]).astype(source.dtype)
    spectral = spectral / modes[None]
    solved = jnp.einsum('ck,mcab->mkab', table_z, spectral, precision=precise)
    solved = jnp.einsum('ai,mkab->mkib', table_x, solved, precision=precise)
    return jnp.einsum('mkib,jb->mkij', solved, table_y, precision=precise)

def tendency(zpadded, x_low, x_high, burning):
    centre = zpadded[:, 2:-2]
    xpadded = jnp.concatenate([x_low[:, :, None, :], centre, x_high[:, :, None, :]], axis=2)
    ypadded = jnp.pad(centre, ((0, 0), (0, 0), (0, 0), (1, 1)))
    east, west = (xpadded[:, :, 2:], xpadded[:, :, :-2])
    north, south = (ypadded[..., 2:], ypadded[..., :-2])
    above, below = (zpadded[:, 3:-1], zpadded[:, 1:-3])
    above_two, below_two = (zpadded[:, 4:], zpadded[:, :-4])
    grad_x = 0.5 * (east - west)
    grad_y = 0.5 * (north - south)
    grad_z = (8.0 * (above - below) - (above_two - below_two)) / 12.0
    laplace = east + west + north + south + above + below - 6.0 * centre
    advection = centre[0] * grad_x + centre[1] * grad_y + centre[2] * grad_z
    reaction = burning * centre[3] * centre[4]
    change = -COURANT * advection + DIFFUSION * laplace
    change = change.at[3].add(-reaction).at[4].add(-STOICHIOMETRY * reaction)
    divergence = grad_x[0] + grad_y[1] + 0.5 * (above[2] - below[2])
    return (change, EXPANSION * reaction - divergence)

def with_ghosts(source, z_low, z_high, x_low, x_high):
    source = source.at[:, 0].add(z_low).at[:, -1].add(z_high)
    return source.at[:, :, 0, :].add(x_low).at[:, :, -1, :].add(x_high)

def correct(fields, pressure, z_low, z_high, x_low, x_high):
    xpadded = jnp.concatenate([x_low[:, None, :], pressure, x_high[:, None, :]], axis=1)
    ypadded = jnp.pad(pressure, ((0, 0), (0, 0), (1, 1)))
    zpadded = jnp.concatenate([z_low[None], pressure, z_high[None]], axis=0)
    grad_x = 0.5 * (xpadded[:, 2:] - xpadded[:, :-2])
    grad_y = 0.5 * (ypadded[..., 2:] - ypadded[..., :-2])
    grad_z = 0.5 * (zpadded[2:] - zpadded[:-2])
    return jnp.concatenate([fields[0:1] - grad_x[None], fields[1:2] - grad_y[None], fields[2:3] - grad_z[None], fields[3:]], axis=0)

def interface(arrays, group):
    return arrays[..., -1, :] if group == 0 else arrays[..., 0, :]

def cross_ghosts(arrays, face_map, group):
    plane = interface(arrays[1 - group], 1 - group)
    flat = plane.reshape((-1, N_MESH, CZ * NY))
    picked = jnp.take_along_axis(flat, jnp.broadcast_to(face_map[group], flat.shape).astype(jnp.int32), axis=-1)
    picked = picked.reshape(plane.shape)
    zeros = jnp.zeros_like(picked)
    return (zeros, picked) if group == 0 else (picked, zeros)

def reference(state, burn_rate, face_map):
    initial = state.reshape(2, FIELDS, NZ, NX, NY)
    burning = burn_rate.reshape(2, NZ, NX, NY)
    current = initial
    pressure = jnp.zeros((2, N_MESH, CZ, NX, NY), state.dtype)
    for section_no in range(SECTIONS):
        predicted = []
        sources = []
        for group in range(2):
            x_low, x_high = cross_ghosts(current, face_map, group)
            zpadded = jnp.pad(current[group], ((0, 0), (2, 2), (0, 0), (0, 0)))
            change, source = tendency(zpadded, x_low, x_high, burning[group])
            if section_no == 0:
                predicted.append(current[group] + change)
            else:
                predicted.append(0.5 * (initial[group] + current[group] + change))
            sources.append(source.reshape(N_MESH, CZ, NX, NY))
        pressure = jnp.zeros((2, N_MESH, CZ, NX, NY), state.dtype)
        zero_layer = jnp.zeros((1, NX, NY), state.dtype)
        for sweep in range(ITERS):
            solved = []
            for group in range(2):
                z_low = jnp.concatenate([zero_layer, pressure[group][:-1, -1]], axis=0)
                z_high = jnp.concatenate([pressure[group][1:, 0], zero_layer], axis=0)
                x_low, x_high = cross_ghosts(pressure, face_map, group)
                solved.append(poisson_solve(with_ghosts(sources[group], z_low, z_high, x_low, x_high)))
            pressure = jnp.stack(solved)
        corrected = []
        for group in range(2):
            x_low, x_high = cross_ghosts(pressure, face_map, group)
            zero_plane = jnp.zeros((NX, NY), state.dtype)
            corrected.append(correct(predicted[group], pressure[group].reshape(NZ, NX, NY), zero_plane, zero_plane, x_low.reshape(NZ, NY), x_high.reshape(NZ, NY)))
        current = jnp.stack(corrected)
    return (current.reshape(2, FIELDS, NZ, NX * NY), pressure.reshape(2, NZ, NX * NY))
```

```python
import functools
import math

import jax
import jax.numpy as jnp
import numpy as np
from jax import lax
from jax.experimental import pallas as pl
from jax.experimental.pallas import tpu as pltpu
from jax.sharding import PartitionSpec as P

NX = 64
NY = 64
FIELDS = 5
SECTIONS = 2
ITERS = 3

COURANT = 0.1
DIFFUSION = 0.05
STOICHIOMETRY = 2.0
EXPANSION = 1.0

LANES = 128
HALF = NY
TILES = NX // 2
ROWS = 32
ZERO_ROW = 8
F32 = jnp.float32
BF16 = jnp.bfloat16


def sine(n):
    i = np.arange(n, dtype=np.float64) + 1
    return np.sqrt(2.0 / (n + 1)) * np.sin(np.pi * i[:, None] * i[None, :] / (n + 1))


def modes(n):
    i = np.arange(n, dtype=np.float64) + 1
    return 2.0 - 2.0 * np.cos(np.pi * i / (n + 1))


def both(low, high):
    return np.concatenate([np.broadcast_to(low, low.shape[:-1] + (HALF,)), np.broadcast_to(high, high.shape[:-1] + (HALF,))], axis=-1)


def split(table):
    table = np.asarray(table, np.float32)
    high = table.astype(BF16)
    low = (table - high.astype(np.float32)).astype(BF16)
    return high, low


def tables(height):
    sz, sx, sy = sine(height), sine(NX), sine(NY)
    lz, lx, ly = modes(height), modes(NX), modes(NY)
    half = height // 2
    coef = both(sz[0::2, :half, None], sz[1::2, :half, None])
    edge = coef[:, 0]
    lam = lx[None, :, None] + both(lz[0::2, None, None], lz[1::2, None, None]) + np.concatenate([ly, ly])[None, None, :]
    inv = 1.0 / lam
    cross = edge[:, None, :] * sx[:, 0][None, :, None] * inv
    diag_z = (edge[:, None, :] ** 2 * inv).sum(0)
    diag_x = (sx[:, 0][None, :, None] ** 2 * inv).sum(1)
    order = np.concatenate([np.arange(0, NX, 2), np.arange(1, NX, 2)])
    fwd_hi, fwd_lo = split(sx[:, order])
    bwd_hi, bwd_lo = split(sx[order, :])
    ky = np.kron(np.eye(2), sy)
    ky_hi, ky_lo = split(ky)
    to_a = np.zeros((half, half, LANES))
    to_b = np.zeros((half, half, LANES))
    from_a = np.zeros((half, half, LANES))
    from_b = np.zeros((half, half, LANES))
    for r in range(half):
        to_a[r] = both(sz[0::2, r][:, None], sz[1::2, half + r][:, None])
        to_b[r] = both(sz[0::2, half + r][:, None], sz[1::2, r][:, None])
        from_a[r] = both(sz[2 * r, :half][:, None], sz[2 * r + 1, half:][:, None])
        from_b[r] = both(sz[2 * r + 1, :half][:, None], sz[2 * r, half:][:, None])
    f = lambda a: np.ascontiguousarray(a, dtype=np.float32)
    return dict(
        coef=f(coef.reshape(half * half, LANES)),
        inv=f(inv),
        cross=f(cross),
        diag_z=f(diag_z),
        diag_x=f(diag_x),
        col_x=f(np.broadcast_to(sx[:, :1], (NX, LANES))),
        edge=f(edge),
        fwd=np.concatenate([fwd_hi, fwd_hi, fwd_lo], axis=1),
        bwd=np.concatenate([bwd_hi, bwd_hi, bwd_lo], axis=1),
        ky2=np.concatenate([ky_hi, ky_hi], axis=0),
        ky_lo=ky_lo,
        plane=f(np.stack([to_a, to_b, from_a, from_b])),
    )


def lower_half(shape):
    return lax.broadcasted_iota(jnp.int32, shape, len(shape) - 1) < HALF


def swap_halves(v):
    return pltpu.roll(v, HALF, axis=v.ndim - 1)


def hi_lo(v):
    high = v.astype(BF16)
    return high, (v - high.astype(F32)).astype(BF16)


def y_transform(v, ky2, ky_lo):
    high, low = hi_lo(v)
    return jnp.dot(jnp.concatenate([high, low], axis=1), ky2[...], preferred_element_type=F32) + jnp.dot(
        high, ky_lo[...], preferred_element_type=F32
    )


def x_transform(table, v):
    high, low = hi_lo(v)
    return jnp.dot(table[...], jnp.concatenate([high, low, high], axis=0), preferred_element_type=F32)


def mix_rows(v, a, b):
    swapped = swap_halves(v)
    out = jnp.zeros_like(v)
    for r in range(v.shape[0]):
        out = out + a[r] * v[r : r + 1] + b[r] * swapped[r : r + 1]
    return out


def gather(plane, mapping):
    half = plane.shape[0]
    bits = int(math.log2(half))
    ybits = int(math.log2(NY))
    row = (mapping >> ybits) & (half - 1)
    lane = ((mapping >> (ybits + bits)) << ybits) | (mapping & (NY - 1))
    out = jnp.zeros_like(plane)
    for r in range(half):
        source = jnp.broadcast_to(plane[r : r + 1], plane.shape)
        out = jnp.where(row == r, jnp.take_along_axis(source, lane, axis=1), out)
    return out


def position():
    is_fine = lax.axis_index("grp") == 0
    even = lax.rem(lax.axis_index("mesh"), 2) == 0
    return is_fine, even


def row_sign(is_fine, shape):
    odd = lax.rem(lax.broadcasted_iota(jnp.int32, shape, 0), 2) == 1
    return jnp.where(jnp.logical_and(odd, is_fine), -1.0, 1.0).astype(F32)


def pack_trace(full):
    n = full.shape[0] // 2
    return jnp.where(lower_half((n, LANES)), full[:n], full[n:])


def unpack_trace(packed):
    swapped = swap_halves(packed)
    low = lower_half(packed.shape)
    return jnp.concatenate([jnp.where(low, packed, swapped), jnp.where(low, swapped, packed)], axis=0)


def send_traces(u, even, to_even, to_odd):
    other = swap_halves(u)
    low = lower_half(u.shape)
    evens = jnp.where(low, u, other)
    odds = jnp.where(low, other, u)
    sign = jnp.where(even, 1.0, -1.0).astype(F32)
    to_even[...] = pack_trace(evens - sign * odds)
    to_odd[...] = pack_trace(evens + sign * odds)


def ghost_low_high(from_even, from_odd, even):
    a, b = unpack_trace(from_even[...]), unpack_trace(from_odd[...])
    return jnp.where(even, b, a), jnp.where(even, a, b)


def send_plane(y, tab, plane_out):
    cells = mix_rows(y_transform(y, tab["ky2"], tab["ky_lo"]), tab["plane"].at[2], tab["plane"].at[3])
    plane_out[...] = cells


def x_ghost_tiles(ghost, is_fine):
    swapped = swap_halves(ghost)
    west = jnp.concatenate([swapped, ghost], axis=0)
    east = jnp.concatenate([ghost, swapped], axis=0)
    zero = jnp.zeros_like(west)
    return jnp.where(is_fine, zero, west), jnp.where(is_fine, east, zero)


def east_west(centre, before, after, low):
    east = swap_halves(jnp.where(low, after, centre))
    west = swap_halves(jnp.where(low, centre, before))
    return east, west


def north_south(centre):
    y = lax.broadcasted_iota(jnp.int32, centre.shape, 1) & (NY - 1)
    north = jnp.where(y == NY - 1, 0.0, pltpu.roll(centre, LANES - 1, axis=1))
    south = jnp.where(y == 0, 0.0, pltpu.roll(centre, 1, axis=1))
    return north, south


def strided(first, count, stride):
    return pl.ds(first, count, stride=stride)


def pack_kernel(height, state, to_even, to_odd, planes):
    is_fine, even = position()
    half = height // 2
    low = lower_half((half, LANES))
    for f in range(FIELDS):
        first = state[f, :, 0:LANES]
        last = state[f, :, (TILES - 1) * LANES : TILES * LANES]
        fine = jnp.where(low, swap_halves(last[:half]), last[half:])
        coarse = jnp.where(low, first[:half], swap_halves(first[half:]))
        planes[f * half : (f + 1) * half] = jnp.where(is_fine, fine, coarse)

    def tile(t, _):
        lanes = pl.ds(pl.multiple_of(t * LANES, LANES), LANES)
        for f in range(FIELDS):
            value = state[f, :, lanes]
            for k in range(2):
                bottom = value[k : k + 1]
                top = value[height - 2 + k : height - 1 + k]
                row = pl.ds((2 * f + k) * TILES + t, 1)
                to_even[row] = jnp.where(even, top, bottom)
                to_odd[row] = jnp.where(even, bottom, top)
        return 0

    lax.fori_loop(0, TILES, tile, 0)


NAMES_SOLVE = ("coef", "inv", "edge", "col_x", "fwd", "ky2", "ky_lo", "plane")


def begin_kernel(height, second, *refs):
    refs = list(refs)
    take = lambda n: [refs.pop(0) for _ in range(n)]
    current, burn, from_even, from_odd, planes, mapping = take(6)
    initial = take(1)[0] if second else None
    tab = dict(zip(NAMES_SOLVE, take(len(NAMES_SOLVE))))
    predicted, spectrum, trace, facet, to_even, to_odd, plane_out = take(7)
    pad, source, folded, mixed = take(4)
    is_fine, even = position()
    half = height // 2
    tile_low = lower_half((height, LANES))

    for f in range(FIELDS):
        ghost = gather(planes[f * half : (f + 1) * half], mapping[...])
        west, east = x_ghost_tiles(ghost, is_fine)
        pad[f, ZERO_ROW : ZERO_ROW + height] = west
        last = (TILES + 1) * ROWS + ZERO_ROW
        pad[f, last : last + height] = east
        for k in range(2):
            rows = slice((2 * f + k) * TILES, (2 * f + k + 1) * TILES)
            below = jnp.where(even, from_odd[rows], from_even[rows])
            above = jnp.where(even, from_even[rows], from_odd[rows])
            pad[f, strided(ROWS + ZERO_ROW - 2 + k, TILES, ROWS)] = below
            pad[f, strided(ROWS + ZERO_ROW + height + k, TILES, ROWS)] = above

    def copy(t, _):
        lanes = pl.ds(pl.multiple_of(t * LANES, LANES), LANES)
        row = pl.multiple_of((t + 1) * ROWS + ZERO_ROW, 8)
        for f in range(FIELDS):
            pad[f, pl.ds(row, height)] = current[f, :, lanes]
        return 0

    lax.fori_loop(0, TILES, copy, 0)

    def tile(t, _):
        lanes = pl.ds(pl.multiple_of(t * LANES, LANES), LANES)
        base = pl.multiple_of((t + 1) * ROWS, ROWS)

        def at(f, dz=0, dt=0):
            window = pad[f, pl.ds(pl.multiple_of(base + dt * ROWS, ROWS), ROWS)]
            return window[ZERO_ROW + dz : ZERO_ROW + dz + height]

        u, v, w = at(0), at(1), at(2)
        fuel, oxygen = at(3), at(4)
        reaction = burn[:, lanes] * fuel * oxygen
        cu = u * (-0.5 * COURANT)
        cv = v * (-0.5 * COURANT)
        cw = w * (-COURANT / 12.0)
        divergence = None
        for f in range(FIELDS):
            centre = (u, v, w, fuel, oxygen)[f]
            east, west = east_west(centre, at(f, 0, -1), at(f, 0, 1), tile_low)
            north, south = north_south(centre)
            above, below = at(f, 1), at(f, -1)
            above_two, below_two = at(f, 2), at(f, -2)
            dx, dy, dz = east - west, north - south, above - below
            change = cu * dx + cv * dy + cw * (8.0 * dz - (above_two - below_two))
            change = change + DIFFUSION * ((east + west) + (north + south) + (above + below) - 6.0 * centre)
            if f == 3:
                change = change - reaction
            if f == 4:
                change = change - STOICHIOMETRY * reaction
            if f == 0:
                divergence = dx
            if f == 1:
                divergence = divergence + dy
            if f == 2:
                divergence = divergence + dz
            if second:
                predicted[f, :, lanes] = 0.5 * (initial[f, :, lanes] + centre + change)
            else:
                predicted[f, :, lanes] = centre + change
        source[pl.ds(pl.multiple_of(t * height, height), height)] = EXPANSION * reaction - 0.5 * divergence
        return 0

    lax.fori_loop(0, TILES, tile, 0)

    low = lower_half((TILES, LANES))
    for q in range(half):
        a = source[strided(q, TILES, height)]
        b = source[strided(height - 1 - q, TILES, height)]
        total, delta = a + b, a - b
        folded[q, 0:TILES] = jnp.where(low, total, swap_halves(delta))
        folded[q, TILES : 2 * TILES] = jnp.where(low, swap_halves(total), delta)

    z_mix(folded, mixed, tab["coef"], half, False)
    wide = jnp.concatenate([mixed[p] for p in range(half)], axis=1)
    wide = x_transform(tab["fwd"], wide)
    tall = jnp.concatenate([wide[:, p * LANES : (p + 1) * LANES] for p in range(half)], axis=0)
    mixed[...] = y_transform(tall, tab["ky2"], tab["ky_lo"]).reshape(half, NX, LANES)

    sign = row_sign(is_fine, (NX, LANES))
    column = tab["col_x"][...] * sign
    u0 = jnp.zeros((NX, LANES), F32)
    for p in range(half):
        solved = mixed[p] * tab["inv"][p]
        spectrum[p] = solved
        u0 = u0 + tab["edge"][p : p + 1] * solved
        facet[p : p + 1] = jnp.sum(column * solved, axis=0, keepdims=True)
    trace[...] = u0
    send_traces(u0, even, to_even, to_odd)
    send_plane(facet[...], tab, plane_out)


def z_mix(src, dst, coef, half, inverse):
    def chunk(r, _):
        rows = pl.ds(pl.multiple_of(r * 8, 8), 8)
        parts = [src[j, rows] for j in range(half)]
        for i in range(half):
            total = None
            for j in range(half):
                k = j * half + i if inverse else i * half + j
                term = coef[k : k + 1] * parts[j]
                total = term if total is None else total + term
            dst[i, rows] = total
        return 0

    lax.fori_loop(0, NX // 8, chunk, 0)


NAMES_STEP = ("cross", "diag_z", "diag_x", "ky2", "ky_lo", "plane")


def ghost_modes(plane, mapping, tab):
    cells = gather(plane[...], mapping[...])
    return y_transform(mix_rows(cells, tab["plane"].at[0], tab["plane"].at[1]), tab["ky2"], tab["ky_lo"])


def step_kernel(height, *refs):
    refs = list(refs)
    take = lambda n: [refs.pop(0) for _ in range(n)]
    from_even, from_odd, plane_in, mapping, trace, facet = take(6)
    tab = dict(zip(NAMES_STEP, take(len(NAMES_STEP))))
    layers_out, side_out, to_even, to_odd, plane_out = take(5)
    (facet_next,) = take(1)
    is_fine, even = position()
    half = height // 2
    low_ghost, high_ghost = ghost_low_high(from_even, from_odd, even)
    layers = jnp.where(lower_half((NX, LANES)), low_ghost + high_ghost, low_ghost - high_ghost)
    side = ghost_modes(plane_in, mapping, tab)
    layers_out[...] = layers
    side_out[...] = side
    sign = row_sign(is_fine, (NX, LANES))
    signed = sign * layers
    cross_sum = jnp.zeros((NX, LANES), F32)
    for p in range(half):
        cross = tab["cross"][p]
        cross_sum = cross_sum + cross * side[p : p + 1]
        facet_next[p : p + 1] = jnp.sum(cross * signed, axis=0, keepdims=True)
    u = trace[...] + tab["diag_z"][...] * layers + sign * cross_sum
    send_traces(u, even, to_even, to_odd)
    send_plane(facet[...] + tab["diag_x"][...] * side + facet_next[...], tab, plane_out)


NAMES_END = ("coef", "inv", "edge", "col_x", "bwd", "ky2", "ky_lo")


def end_kernel(height, final, *refs):
    refs = list(refs)
    take = lambda n: [refs.pop(0) for _ in range(n)]
    from_even, from_odd, plane_in, mapping, spectrum, layers, side, predicted = take(8)
    tab = dict(zip(NAMES_END, take(len(NAMES_END))))
    state = take(1)[0]
    if final:
        (head,) = take(1)
    else:
        to_even, to_odd, planes = take(3)
    tall, mixed, unmixed, pad = take(4)
    is_fine, even = position()
    half = height // 2
    sign = row_sign(is_fine, (NX, LANES))
    column = tab["col_x"][...] * sign
    for p in range(half):
        push = tab["edge"][p : p + 1] * layers[...] + column * side[p : p + 1]
        tall[p * NX : (p + 1) * NX] = spectrum[p] + push * tab["inv"][p]
    low_ghost, high_ghost = ghost_low_high(from_even, from_odd, even)
    tall[half * NX : (half + 1) * NX] = jnp.where(lower_half((NX, LANES)), low_ghost, high_ghost)

    cells = y_transform(tall[...], tab["ky2"], tab["ky_lo"])
    wide = jnp.concatenate([cells[p * NX : (p + 1) * NX] for p in range(half + 1)], axis=1)
    wide = x_transform(tab["bwd"], wide)
    for p in range(half):
        mixed[p] = wide[:, p * LANES : (p + 1) * LANES]
    z_mix(mixed, unmixed, tab["coef"], half, True)

    low = lower_half((TILES, LANES))

    def unfold(v):
        top, bottom = v[:TILES], v[TILES:]
        return jnp.where(low, top, swap_halves(bottom)), jnp.where(low, swap_halves(top), bottom)

    first = ROWS + ZERO_ROW
    below, above = unfold(wide[:, half * LANES : (half + 1) * LANES])
    pad[strided(first - 1, TILES, ROWS)] = below
    pad[strided(first + height, TILES, ROWS)] = above
    for q in range(half):
        evens, odds = unfold(unmixed[q])
        pad[strided(first + q, TILES, ROWS)] = evens + odds
        pad[strided(first + height - 1 - q, TILES, ROWS)] = evens - odds
    west, east = x_ghost_tiles(gather(plane_in[...], mapping[...]), is_fine)
    pad[ZERO_ROW : ZERO_ROW + height] = west
    last = (TILES + 1) * ROWS + ZERO_ROW
    pad[last : last + height] = east

    tile_low = lower_half((height, LANES))

    def tile(t, _):
        lanes = pl.ds(pl.multiple_of(t * LANES, LANES), LANES)
        base = pl.multiple_of((t + 1) * ROWS, ROWS)

        def at(dz=0, dt=0):
            window = pad[pl.ds(pl.multiple_of(base + dt * ROWS, ROWS), ROWS)]
            return window[ZERO_ROW + dz : ZERO_ROW + dz + height]

        centre = at()
        east, west = east_west(centre, at(0, -1), at(0, 1), tile_low)
        north, south = north_south(centre)
        slopes = (east - west, north - south, at(1) - at(-1))
        for f in range(FIELDS):
            value = predicted[f, :, lanes]
            if f < 3:
                value = value - 0.5 * slopes[f]
            state[f, :, lanes] = value
            if not final:
                for k in range(2):
                    bottom = value[k : k + 1]
                    top = value[height - 2 + k : height - 1 + k]
                    row = pl.ds((2 * f + k) * TILES + t, 1)
                    to_even[row] = jnp.where(even, top, bottom)
                    to_odd[row] = jnp.where(even, bottom, top)
        if final:
            head[:, lanes] = centre
        return 0

    lax.fori_loop(0, TILES, tile, 0)
    if not final:
        half_low = lower_half((half, LANES))
        for f in range(FIELDS):
            first = state[f, :, 0:LANES]
            last = state[f, :, (TILES - 1) * LANES : TILES * LANES]
            fine = jnp.where(half_low, swap_halves(last[:half]), last[half:])
            coarse = jnp.where(half_low, first[:half], swap_halves(first[half:]))
            planes[f * half : (f + 1) * half] = jnp.where(is_fine, fine, coarse)


def swap_pairs(x, parity):
    count = lax.axis_size("mesh")
    route = []
    for low in range(parity, count - 1, 2):
        route += [(low, low + 1), (low + 1, low)]
    return lax.ppermute(x, "mesh", route)


def swap_partner(x):
    return lax.ppermute(x, "grp", [(0, 1), (1, 0)])


def exchange(to_even, to_odd, plane):
    return swap_pairs(to_even, 0), swap_pairs(to_odd, 1), swap_partner(plane)


def shards(state, burn_rate, face_map):
    height = state.shape[2]
    half = height // 2
    cells = NX * NY
    tab = {name: jnp.asarray(value) for name, value in tables(height).items()}
    shape = lambda *s: jax.ShapeDtypeStruct(s, F32)
    halo = shape(2 * FIELDS * TILES, LANES)
    trace_packed = shape(NX // 2, LANES)
    plane = shape(half, LANES)
    initial = state[0]
    burning = burn_rate[0]
    by_row = face_map[0, 0].reshape(height, NY)
    mapping = jnp.concatenate([by_row[:half], by_row[half:]], axis=1)

    to_even, to_odd, planes = pl.pallas_call(
        functools.partial(pack_kernel, height),
        out_shape=(halo, halo, shape(FIELDS * half, LANES)),
        name="pack",
    )(initial)
    current = initial
    for section in range(SECTIONS):
        second = section > 0
        final = section == SECTIONS - 1
        from_even, from_odd, planes_in = exchange(to_even, to_odd, planes)
        args = (current, burning, from_even, from_odd, planes_in, mapping) + ((initial,) if second else ())
        predicted, spectrum, trace, facet, to_even, to_odd, plane_out = pl.pallas_call(
            functools.partial(begin_kernel, height, second),
            out_shape=(
                shape(FIELDS, height, cells),
                shape(half, NX, LANES),
                shape(NX, LANES),
                plane,
                trace_packed,
                trace_packed,
                plane,
            ),
            scratch_shapes=[
                pltpu.VMEM((FIELDS, (TILES + 2) * ROWS, LANES), F32),
                pltpu.VMEM((TILES * height, LANES), F32),
                pltpu.VMEM((half, NX, LANES), F32),
                pltpu.VMEM((half, NX, LANES), F32),
            ],
            name="begin",
        )(*args, *(tab[n] for n in NAMES_SOLVE))
        for _ in range(ITERS - 1):
            received = exchange(to_even, to_odd, plane_out)
            layers, side, to_even, to_odd, plane_out = pl.pallas_call(
                functools.partial(step_kernel, height),
                out_shape=(shape(NX, LANES), plane, trace_packed, trace_packed, plane),
                scratch_shapes=[pltpu.VMEM((half, LANES), F32)],
                name="step",
            )(*received, mapping, trace, facet, *(tab[n] for n in NAMES_STEP))
        received = exchange(to_even, to_odd, plane_out)
        outs = pl.pallas_call(
            functools.partial(end_kernel, height, final),
            out_shape=(shape(FIELDS, height, cells),)
            + ((shape(height, cells),) if final else (halo, halo, shape(FIELDS * half, LANES))),
            scratch_shapes=[
                pltpu.VMEM(((half + 1) * NX, LANES), F32),
                pltpu.VMEM((half, NX, LANES), F32),
                pltpu.VMEM((half, NX, LANES), F32),
                pltpu.VMEM(((TILES + 2) * ROWS, LANES), F32),
            ],
            name="end",
        )(*received, mapping, spectrum, layers, side, predicted, *(tab[n] for n in NAMES_END))
        current = outs[0]
        if not final:
            to_even, to_odd, planes = outs[1:]
    return current[None], outs[1][None]


def solution(mesh):
    placed = (P("grp", None, "mesh", None), P("grp", "mesh", None), P("grp", "mesh", None))
    return jax.shard_map(
        shards,
        mesh=mesh,
        in_specs=placed,
        out_specs=(P("grp", None, "mesh", None), P("grp", "mesh", None)),
        check_vma=False,
    )
```

```python
import functools
import math

import jax
import jax.numpy as jnp
import numpy as np
from jax import lax
from jax.experimental import pallas as pl
from jax.experimental.pallas import tpu as pltpu
from jax.sharding import PartitionSpec as P

NX = 64
NY = 64
FIELDS = 5
SECTIONS = 2
ITERS = 3

COURANT = 0.1
DIFFUSION = 0.05
STOICHIOMETRY = 2.0
EXPANSION = 1.0

LANES = 128
HALF = NY
TILES = NX // 2
ROWS = 32
ZERO_ROW = 8
F32 = jnp.float32
BF16 = jnp.bfloat16
MIB = 1 << 20


def sine(n):
    i = np.arange(n, dtype=np.float64) + 1
    return np.sqrt(2.0 / (n + 1)) * np.sin(np.pi * i[:, None] * i[None, :] / (n + 1))


def modes(n):
    i = np.arange(n, dtype=np.float64) + 1
    return 2.0 - 2.0 * np.cos(np.pi * i / (n + 1))


def both(low, high):
    return np.concatenate([np.broadcast_to(low, low.shape[:-1] + (HALF,)), np.broadcast_to(high, high.shape[:-1] + (HALF,))], axis=-1)


def split(table):
    table = np.asarray(table, np.float32)
    high = table.astype(BF16)
    low = (table - high.astype(np.float32)).astype(BF16)
    return high, low


def tables(height):
    sz, sx, sy = sine(height), sine(NX), sine(NY)
    lz, lx, ly = modes(height), modes(NX), modes(NY)
    half = height // 2
    coef = both(sz[0::2, :half, None], sz[1::2, :half, None])
    edge = coef[:, 0]
    lam = lx[None, :, None] + both(lz[0::2, None, None], lz[1::2, None, None]) + np.concatenate([ly, ly])[None, None, :]
    inv = 1.0 / lam
    cross = edge[:, None, :] * sx[:, 0][None, :, None] * inv
    diag_z = (edge[:, None, :] ** 2 * inv).sum(0)
    diag_x = (sx[:, 0][None, :, None] ** 2 * inv).sum(1)
    order = np.concatenate([np.arange(0, NX, 2), np.arange(1, NX, 2)])
    fwd_hi, fwd_lo = split(sx[:, order])
    bwd_hi, bwd_lo = split(sx[order, :])
    ky = np.kron(np.eye(2), sy)
    ky_hi, ky_lo = split(ky)
    to_a = np.zeros((half, half, LANES))
    to_b = np.zeros((half, half, LANES))
    from_a = np.zeros((half, half, LANES))
    from_b = np.zeros((half, half, LANES))
    for r in range(half):
        to_a[r] = both(sz[0::2, r][:, None], sz[1::2, half + r][:, None])
        to_b[r] = both(sz[0::2, half + r][:, None], sz[1::2, r][:, None])
        from_a[r] = both(sz[2 * r, :half][:, None], sz[2 * r + 1, half:][:, None])
        from_b[r] = both(sz[2 * r + 1, :half][:, None], sz[2 * r, half:][:, None])
    hi = lambda high, low: np.concatenate([high, high, low, np.zeros_like(low)], axis=1)
    wide = lambda m: np.concatenate([m[:, :LANES], m[:, LANES:]], axis=0)
    parts = dict(
        coef=coef.reshape(half * half, LANES),
        inv=inv.reshape(half * NX, LANES),
        cross=cross.reshape(half * NX, LANES),
        diag_z=diag_z,
        diag_x=diag_x,
        col_x=np.broadcast_to(sx[:, :1], (NX, LANES)),
        edge=edge,
        fwd=wide(hi(fwd_hi, fwd_lo)),
        bwd=wide(hi(bwd_hi, bwd_lo)),
        ky_hi=ky_hi,
        ky_lo=ky_lo,
        plane=np.stack([to_a, to_b, from_a, from_b]).reshape(4 * half * half, LANES),
    )
    places, at = {}, 0
    for name, part in parts.items():
        places[name] = (at, at + part.shape[0])
        at += part.shape[0]
    return np.concatenate([np.asarray(p, np.float32) for p in parts.values()], axis=0), places


class Tables:
    def __init__(self, ref, places):
        self.ref, self.places = ref, places

    def __getitem__(self, name):
        first, last = self.places[name]
        return self.ref[first:last]

    def row(self, name, i):
        first = self.places[name][0] + i
        return self.ref[first : first + 1]

    def block(self, name, i, n):
        first = self.places[name][0] + i * n
        return self.ref[first : first + n]

    def wide(self, name):
        both_halves = self[name].astype(BF16)
        n = both_halves.shape[0] // 2
        return jnp.concatenate([both_halves[:n], both_halves[n:]], axis=1)


def lower_half(shape):
    return lax.broadcasted_iota(jnp.int32, shape, len(shape) - 1) < HALF


def swap_halves(v):
    return pltpu.roll(v, HALF, axis=v.ndim - 1)


def hi_lo(v):
    high = v.astype(BF16)
    return high, (v - high.astype(F32)).astype(BF16)


def y_transform(v, tab):
    high, low = hi_lo(v)
    table = tab["ky_hi"].astype(BF16)
    return jnp.dot(
        jnp.concatenate([high, low], axis=1), jnp.concatenate([table, table], axis=0), preferred_element_type=F32
    ) + jnp.dot(high, tab["ky_lo"].astype(BF16), preferred_element_type=F32)


def x_transform(table, v):
    high, low = hi_lo(v)
    return jnp.dot(table, jnp.concatenate([high, low, high, jnp.zeros_like(high)], axis=0), preferred_element_type=F32)


def mix_rows(v, tab, first):
    swapped = swap_halves(v)
    half = v.shape[0]
    out = jnp.zeros_like(v)
    for r in range(half):
        a = tab.block("plane", first * half + r, half)
        b = tab.block("plane", (first + 1) * half + r, half)
        out = out + a * v[r : r + 1] + b * swapped[r : r + 1]
    return out


def gather(plane, mapping):
    half = plane.shape[0]
    bits = int(math.log2(half))
    ybits = int(math.log2(NY))
    row = (mapping >> ybits) & (half - 1)
    lane = ((mapping >> (ybits + bits)) << ybits) | (mapping & (NY - 1))
    out = jnp.zeros_like(plane)
    for r in range(half):
        source = jnp.broadcast_to(plane[r : r + 1], plane.shape)
        out = jnp.where(row == r, jnp.take_along_axis(source, lane, axis=1), out)
    return out


def position():
    is_fine = lax.axis_index("grp") == 0
    even = lax.rem(lax.axis_index("mesh"), 2) == 0
    return is_fine, even


def row_sign(is_fine, shape):
    odd = lax.rem(lax.broadcasted_iota(jnp.int32, shape, 0), 2) == 1
    return jnp.where(jnp.logical_and(odd, is_fine), -1.0, 1.0).astype(F32)


def pack_trace(full):
    n = full.shape[0] // 2
    return jnp.where(lower_half((n, LANES)), full[:n], full[n:])


def unpack_trace(packed):
    swapped = swap_halves(packed)
    low = lower_half(packed.shape)
    return jnp.concatenate([jnp.where(low, packed, swapped), jnp.where(low, swapped, packed)], axis=0)


def send_traces(u, even, to_even, to_odd):
    other = swap_halves(u)
    low = lower_half(u.shape)
    evens = jnp.where(low, u, other)
    odds = jnp.where(low, other, u)
    sign = jnp.where(even, 1.0, -1.0).astype(F32)
    to_even[...] = pack_trace(evens - sign * odds)
    to_odd[...] = pack_trace(evens + sign * odds)


def ghost_low_high(from_even, from_odd, even):
    a, b = unpack_trace(from_even[...]), unpack_trace(from_odd[...])
    return jnp.where(even, b, a), jnp.where(even, a, b)


def send_plane(y, tab, plane_out):
    plane_out[...] = mix_rows(y_transform(y, tab), tab, 2)


def x_ghost_tiles(ghost, is_fine):
    swapped = swap_halves(ghost)
    west = jnp.concatenate([swapped, ghost], axis=0)
    east = jnp.concatenate([ghost, swapped], axis=0)
    zero = jnp.zeros_like(west)
    return jnp.where(is_fine, zero, west), jnp.where(is_fine, east, zero)


def east_west(centre, before, after, low):
    east = swap_halves(jnp.where(low, after, centre))
    west = swap_halves(jnp.where(low, centre, before))
    return east, west


def north_south(centre):
    y = lax.broadcasted_iota(jnp.int32, centre.shape, 1) & (NY - 1)
    north = jnp.where(y == NY - 1, 0.0, pltpu.roll(centre, LANES - 1, axis=1))
    south = jnp.where(y == 0, 0.0, pltpu.roll(centre, 1, axis=1))
    return north, south


def strided(first, count, stride):
    return pl.ds(first, count, stride=stride)


def pack_kernel(height, state, to_even, to_odd, planes):
    is_fine, even = position()
    half = height // 2
    low = lower_half((half, LANES))
    for f in range(FIELDS):
        first = state[f, :, 0:LANES]
        last = state[f, :, (TILES - 1) * LANES : TILES * LANES]
        fine = jnp.where(low, swap_halves(last[:half]), last[half:])
        coarse = jnp.where(low, first[:half], swap_halves(first[half:]))
        planes[f * half : (f + 1) * half] = jnp.where(is_fine, fine, coarse)

    def tile(t, _):
        lanes = pl.ds(pl.multiple_of(t * LANES, LANES), LANES)
        for f in range(FIELDS):
            value = state[f, :, lanes]
            for k in range(2):
                bottom = value[k : k + 1]
                top = value[height - 2 + k : height - 1 + k]
                row = pl.ds((2 * f + k) * TILES + t, 1)
                to_even[row] = jnp.where(even, top, bottom)
                to_odd[row] = jnp.where(even, bottom, top)
        return 0

    lax.fori_loop(0, TILES, tile, 0)


def begin_kernel(height, places, second, *refs):
    refs = list(refs)
    take = lambda n: [refs.pop(0) for _ in range(n)]
    current, burn, from_even, from_odd, planes, mapping = take(6)
    initial = take(1)[0] if second else None
    tab = Tables(take(1)[0], places)
    predicted, spectrum, trace, facet, to_even, to_odd, plane_out = take(7)
    pad, source, folded, mixed = take(4)
    is_fine, even = position()
    half = height // 2
    tile_low = lower_half((height, LANES))
    tiled = pad.reshape(FIELDS, TILES + 2, ROWS, LANES)

    for f in range(FIELDS):
        ghost = gather(planes[f * half : (f + 1) * half], mapping[...])
        west, east = x_ghost_tiles(ghost, is_fine)
        pad[f, ZERO_ROW : ZERO_ROW + height] = west
        last = (TILES + 1) * ROWS + ZERO_ROW
        pad[f, last : last + height] = east
        for k in range(2):
            rows = slice((2 * f + k) * TILES, (2 * f + k + 1) * TILES)
            below = jnp.where(even, from_odd[rows], from_even[rows])
            above = jnp.where(even, from_even[rows], from_odd[rows])
            pad[f, strided(ROWS + ZERO_ROW - 2 + k, TILES, ROWS)] = below
            pad[f, strided(ROWS + ZERO_ROW + height + k, TILES, ROWS)] = above

    def copy(t, _):
        lanes = pl.ds(pl.multiple_of(t * LANES, LANES), LANES)
        row = pl.multiple_of((t + 1) * ROWS + ZERO_ROW, 8)
        for f in range(FIELDS):
            pad[f, pl.ds(row, height)] = current[f, :, lanes]
        return 0

    lax.fori_loop(0, TILES, copy, 0)

    def tile(t, _):
        lanes = pl.ds(pl.multiple_of(t * LANES, LANES), LANES)

        def at(f, dz=0, dt=0):
            return tiled[f, t + 1 + dt, ZERO_ROW + dz : ZERO_ROW + dz + height]

        u, v, w = at(0), at(1), at(2)
        fuel, oxygen = at(3), at(4)
        reaction = burn[:, lanes] * fuel * oxygen
        cu = u * (-0.5 * COURANT)
        cv = v * (-0.5 * COURANT)
        cw = w * (-COURANT / 12.0)
        divergence = None
        for f in range(FIELDS):
            centre = (u, v, w, fuel, oxygen)[f]
            east, west = east_west(centre, at(f, 0, -1), at(f, 0, 1), tile_low)
            north, south = north_south(centre)
            above, below = at(f, 1), at(f, -1)
            above_two, below_two = at(f, 2), at(f, -2)
            dx, dy, dz = east - west, north - south, above - below
            change = cu * dx + cv * dy + cw * (8.0 * dz - (above_two - below_two))
            change = change + DIFFUSION * ((east + west) + (north + south) + (above + below) - 6.0 * centre)
            if f == 3:
                change = change - reaction
            if f == 4:
                change = change - STOICHIOMETRY * reaction
            if f == 0:
                divergence = dx
            if f == 1:
                divergence = divergence + dy
            if f == 2:
                divergence = divergence + dz
            if second:
                predicted[f, :, lanes] = 0.5 * (initial[f, :, lanes] + centre + change)
            else:
                predicted[f, :, lanes] = centre + change
        source[pl.ds(pl.multiple_of(t * height, height), height)] = EXPANSION * reaction - 0.5 * divergence
        return 0

    lax.fori_loop(0, TILES, tile, 0)

    low = lower_half((TILES, LANES))
    for q in range(half):
        a = source[strided(q, TILES, height)]
        b = source[strided(height - 1 - q, TILES, height)]
        total, delta = a + b, a - b
        folded[q, 0:TILES] = jnp.where(low, total, swap_halves(delta))
        folded[q, TILES : 2 * TILES] = jnp.where(low, swap_halves(total), delta)

    z_mix(folded, mixed, tab, half, False)
    wide = jnp.concatenate([mixed[p] for p in range(half)], axis=1)
    wide = x_transform(tab.wide("fwd"), wide)
    tall = jnp.concatenate([wide[:, p * LANES : (p + 1) * LANES] for p in range(half)], axis=0)
    mixed[...] = y_transform(tall, tab).reshape(half, NX, LANES)

    sign = row_sign(is_fine, (NX, LANES))
    column = tab["col_x"] * sign
    u0 = jnp.zeros((NX, LANES), F32)
    for p in range(half):
        solved = mixed[p] * tab.block("inv", p, NX)
        spectrum[p] = solved
        u0 = u0 + tab.row("edge", p) * solved
        facet[p : p + 1] = jnp.sum(column * solved, axis=0, keepdims=True)
    trace[...] = u0
    send_traces(u0, even, to_even, to_odd)
    send_plane(facet[...], tab, plane_out)


def z_mix(src, dst, tab, half, inverse):
    def chunk(r, _):
        rows = pl.ds(pl.multiple_of(r * 8, 8), 8)
        parts = [src[j, rows] for j in range(half)]
        for i in range(half):
            total = None
            for j in range(half):
                k = j * half + i if inverse else i * half + j
                term = tab.row("coef", k) * parts[j]
                total = term if total is None else total + term
            dst[i, rows] = total
        return 0

    lax.fori_loop(0, NX // 8, chunk, 0)


def ghost_modes(plane, mapping, tab):
    cells = gather(plane[...], mapping[...])
    return y_transform(mix_rows(cells, tab, 0), tab)


def step_kernel(height, places, last, *refs):
    refs = list(refs)
    take = lambda n: [refs.pop(0) for _ in range(n)]
    from_even, from_odd, plane_in, mapping, trace, facet = take(6)
    tab = Tables(take(1)[0], places)
    layers_out, side_out = take(2) if last else (None, None)
    to_even, to_odd, plane_out = take(3)
    (facet_next,) = take(1)
    is_fine, even = position()
    half = height // 2
    low_ghost, high_ghost = ghost_low_high(from_even, from_odd, even)
    layers = jnp.where(lower_half((NX, LANES)), low_ghost + high_ghost, low_ghost - high_ghost)
    side = ghost_modes(plane_in, mapping, tab)
    if last:
        layers_out[...] = layers
        side_out[...] = side
    sign = row_sign(is_fine, (NX, LANES))
    signed = sign * layers
    cross_sum = jnp.zeros((NX, LANES), F32)
    for p in range(half):
        cross = tab.block("cross", p, NX)
        cross_sum = cross_sum + cross * side[p : p + 1]
        facet_next[p : p + 1] = jnp.sum(cross * signed, axis=0, keepdims=True)
    u = trace[...] + tab["diag_z"] * layers + sign * cross_sum
    send_traces(u, even, to_even, to_odd)
    send_plane(facet[...] + tab["diag_x"] * side + facet_next[...], tab, plane_out)


def end_kernel(height, places, final, *refs):
    refs = list(refs)
    take = lambda n: [refs.pop(0) for _ in range(n)]
    from_even, from_odd, plane_in, mapping, spectrum, layers, side, predicted = take(8)
    tab = Tables(take(1)[0], places)
    state = take(1)[0]
    if final:
        (head,) = take(1)
    else:
        to_even, to_odd, planes = take(3)
    tall, mixed, unmixed, pad = take(4)
    is_fine, even = position()
    half = height // 2
    sign = row_sign(is_fine, (NX, LANES))
    column = tab["col_x"] * sign
    for p in range(half):
        push = tab.row("edge", p) * layers[...] + column * side[p : p + 1]
        tall[p * NX : (p + 1) * NX] = spectrum[p] + push * tab.block("inv", p, NX)
    low_ghost, high_ghost = ghost_low_high(from_even, from_odd, even)
    tall[half * NX : (half + 1) * NX] = jnp.where(lower_half((NX, LANES)), low_ghost, high_ghost)

    cells = y_transform(tall[...], tab)
    wide = jnp.concatenate([cells[p * NX : (p + 1) * NX] for p in range(half + 1)], axis=1)
    wide = x_transform(tab.wide("bwd"), wide)
    for p in range(half):
        mixed[p] = wide[:, p * LANES : (p + 1) * LANES]
    z_mix(mixed, unmixed, tab, half, True)

    low = lower_half((TILES, LANES))

    def unfold(v):
        top, bottom = v[:TILES], v[TILES:]
        return jnp.where(low, top, swap_halves(bottom)), jnp.where(low, swap_halves(top), bottom)

    first = ROWS + ZERO_ROW
    below, above = unfold(wide[:, half * LANES : (half + 1) * LANES])
    pad[strided(first - 1, TILES, ROWS)] = below
    pad[strided(first + height, TILES, ROWS)] = above
    for q in range(half):
        evens, odds = unfold(unmixed[q])
        pad[strided(first + q, TILES, ROWS)] = evens + odds
        pad[strided(first + height - 1 - q, TILES, ROWS)] = evens - odds
    west, east = x_ghost_tiles(gather(plane_in[...], mapping[...]), is_fine)
    pad[ZERO_ROW : ZERO_ROW + height] = west
    last = (TILES + 1) * ROWS + ZERO_ROW
    pad[last : last + height] = east

    tile_low = lower_half((height, LANES))
    tiled = pad.reshape(TILES + 2, ROWS, LANES)

    def tile(t, _):
        lanes = pl.ds(pl.multiple_of(t * LANES, LANES), LANES)

        def at(dz=0, dt=0):
            return tiled[t + 1 + dt, ZERO_ROW + dz : ZERO_ROW + dz + height]

        centre = at()
        east, west = east_west(centre, at(0, -1), at(0, 1), tile_low)
        north, south = north_south(centre)
        slopes = (east - west, north - south, at(1) - at(-1))
        for f in range(FIELDS):
            value = predicted[f, :, lanes]
            if f < 3:
                value = value - 0.5 * slopes[f]
            state[f, :, lanes] = value
            if not final:
                for k in range(2):
                    bottom = value[k : k + 1]
                    top = value[height - 2 + k : height - 1 + k]
                    row = pl.ds((2 * f + k) * TILES + t, 1)
                    to_even[row] = jnp.where(even, top, bottom)
                    to_odd[row] = jnp.where(even, bottom, top)
        if final:
            head[:, lanes] = centre
        return 0

    lax.fori_loop(0, TILES, tile, 0)
    if not final:
        half_low = lower_half((half, LANES))
        for f in range(FIELDS):
            first = state[f, :, 0:LANES]
            last = state[f, :, (TILES - 1) * LANES : TILES * LANES]
            fine = jnp.where(half_low, swap_halves(last[:half]), last[half:])
            coarse = jnp.where(half_low, first[:half], swap_halves(first[half:]))
            planes[f * half : (f + 1) * half] = jnp.where(is_fine, fine, coarse)


def swap_pairs(x, parity):
    count = lax.axis_size("mesh")
    route = []
    for low in range(parity, count - 1, 2):
        route += [(low, low + 1), (low + 1, low)]
    return lax.ppermute(x, "mesh", route)


def swap_partner(x):
    return lax.ppermute(x, "grp", [(0, 1), (1, 0)])


def exchange(to_even, to_odd, plane):
    return swap_pairs(to_even, 0), swap_pairs(to_odd, 1), swap_partner(plane)


def shards(state, burn_rate, face_map):
    height = state.shape[2]
    half = height // 2
    cells = NX * NY
    table, places = tables(height)
    table = jnp.asarray(table)
    shape = lambda *s: jax.ShapeDtypeStruct(s, F32)
    halo = shape(2 * FIELDS * TILES, LANES)
    trace_packed = shape(NX // 2, LANES)
    plane = shape(half, LANES)
    initial = state[0]
    burning = burn_rate[0]
    by_row = face_map[0, 0].reshape(height, NY)
    mapping = jnp.concatenate([by_row[:half], by_row[half:]], axis=1)

    to_even, to_odd, planes = pl.pallas_call(
        functools.partial(pack_kernel, height),
        out_shape=(halo, halo, shape(FIELDS * half, LANES)),
        compiler_params=pltpu.CompilerParams(vmem_limit_bytes=8 * MIB),
        name="pack",
    )(initial)
    current = initial
    for section in range(SECTIONS):
        second = section > 0
        final = section == SECTIONS - 1
        from_even, from_odd, planes_in = exchange(to_even, to_odd, planes)
        args = (current, burning, from_even, from_odd, planes_in, mapping) + ((initial,) if second else ())
        predicted, spectrum, trace, facet, to_even, to_odd, plane_out = pl.pallas_call(
            functools.partial(begin_kernel, height, places, second),
            out_shape=(
                shape(FIELDS, height, cells),
                shape(half, NX, LANES),
                shape(NX, LANES),
                plane,
                trace_packed,
                trace_packed,
                plane,
            ),
            scratch_shapes=[
                pltpu.VMEM((FIELDS, (TILES + 2) * ROWS, LANES), F32),
                pltpu.VMEM((TILES * height, LANES), F32),
                pltpu.VMEM((half, NX, LANES), F32),
                pltpu.VMEM((half, NX, LANES), F32),
            ],
            compiler_params=pltpu.CompilerParams(vmem_limit_bytes=16 * MIB),
            name="begin",
        )(*args, table)
        for sweep in range(ITERS - 1):
            last = sweep == ITERS - 2
            received = exchange(to_even, to_odd, plane_out)
            *kept, to_even, to_odd, plane_out = pl.pallas_call(
                functools.partial(step_kernel, height, places, last),
                out_shape=((shape(NX, LANES), plane) if last else ()) + (trace_packed, trace_packed, plane),
                scratch_shapes=[pltpu.VMEM((half, LANES), F32)],
                compiler_params=pltpu.CompilerParams(vmem_limit_bytes=4 * MIB),
                name="step",
            )(*received, mapping, trace, facet, table)
        received = exchange(to_even, to_odd, plane_out)
        outs = pl.pallas_call(
            functools.partial(end_kernel, height, places, final),
            out_shape=(shape(FIELDS, height, cells),)
            + ((shape(height, cells),) if final else (halo, halo, shape(FIELDS * half, LANES))),
            scratch_shapes=[
                pltpu.VMEM(((half + 1) * NX, LANES), F32),
                pltpu.VMEM((half, NX, LANES), F32),
                pltpu.VMEM((half, NX, LANES), F32),
                pltpu.VMEM(((TILES + 2) * ROWS, LANES), F32),
            ],
            compiler_params=pltpu.CompilerParams(vmem_limit_bytes=16 * MIB),
            name="end",
        )(*received, mapping, spectrum, *kept, predicted, table)
        current = outs[0]
        if not final:
            to_even, to_odd, planes = outs[1:]
    return current[None], outs[1][None]


def solution(mesh):
    placed = (P("grp", None, "mesh", None), P("grp", "mesh", None), P("grp", "mesh", None))
    return jax.shard_map(
        shards,
        mesh=mesh,
        in_specs=placed,
        out_specs=(P("grp", None, "mesh", None), P("grp", "mesh", None)),
        check_vma=False,
    )
```

```python
import functools
import math

import jax
import jax.numpy as jnp
import numpy as np
from jax import lax
from jax.experimental import pallas as pl
from jax.experimental.pallas import tpu as pltpu
from jax.sharding import PartitionSpec as P

NX = 64
NY = 64
FIELDS = 5
SECTIONS = 2
ITERS = 3

COURANT = 0.1
DIFFUSION = 0.05
STOICHIOMETRY = 2.0
EXPANSION = 1.0

LANES = 128
HALF = NY
TILES = NX // 2
ROWS = 32
ZERO_ROW = 8
F32 = jnp.float32
BF16 = jnp.bfloat16
UNROLL = 16
MIB = 1 << 20
MICROSECOND = 8_000_000


def sine(n):
    i = np.arange(n, dtype=np.float64) + 1
    return np.sqrt(2.0 / (n + 1)) * np.sin(np.pi * i[:, None] * i[None, :] / (n + 1))


def modes(n):
    i = np.arange(n, dtype=np.float64) + 1
    return 2.0 - 2.0 * np.cos(np.pi * i / (n + 1))


def both(low, high):
    return np.concatenate([np.broadcast_to(low, low.shape[:-1] + (HALF,)), np.broadcast_to(high, high.shape[:-1] + (HALF,))], axis=-1)


def split(table):
    table = np.asarray(table, np.float32)
    high = table.astype(BF16)
    low = (table - high.astype(np.float32)).astype(BF16)
    return high, low


def tables(height):
    sz, sx, sy = sine(height), sine(NX), sine(NY)
    lz, lx, ly = modes(height), modes(NX), modes(NY)
    half = height // 2
    coef = both(sz[0::2, :half, None], sz[1::2, :half, None])
    edge = coef[:, 0]
    lam = lx[None, :, None] + both(lz[0::2, None, None], lz[1::2, None, None]) + np.concatenate([ly, ly])[None, None, :]
    inv = 1.0 / lam
    cross = edge[:, None, :] * sx[:, 0][None, :, None] * inv
    diag_z = (edge[:, None, :] ** 2 * inv).sum(0)
    diag_x = (sx[:, 0][None, :, None] ** 2 * inv).sum(1)
    order = np.concatenate([np.arange(0, NX, 2), np.arange(1, NX, 2)])
    fwd_hi, fwd_lo = split(sx[:, order])
    bwd_hi, bwd_lo = split(sx[order, :])
    ky = np.kron(np.eye(2), sy)
    ky_hi, ky_lo = split(ky)
    to_a = np.zeros((half, half, LANES))
    to_b = np.zeros((half, half, LANES))
    from_a = np.zeros((half, half, LANES))
    from_b = np.zeros((half, half, LANES))
    for r in range(half):
        to_a[r] = both(sz[0::2, r][:, None], sz[1::2, half + r][:, None])
        to_b[r] = both(sz[0::2, half + r][:, None], sz[1::2, r][:, None])
        from_a[r] = both(sz[2 * r, :half][:, None], sz[2 * r + 1, half:][:, None])
        from_b[r] = both(sz[2 * r + 1, :half][:, None], sz[2 * r, half:][:, None])
    hi = lambda high, low: np.concatenate([high, high, low, np.zeros_like(low)], axis=1)
    wide = lambda m: np.concatenate([m[:, :LANES], m[:, LANES:]], axis=0)
    parts = dict(
        coef=coef.reshape(half * half, LANES),
        inv=inv.reshape(half * NX, LANES),
        cross=cross.reshape(half * NX, LANES),
        diag_z=diag_z,
        diag_x=diag_x,
        col_x=np.broadcast_to(sx[:, :1], (NX, LANES)),
        edge=edge,
        fwd=wide(hi(fwd_hi, fwd_lo)),
        bwd=wide(hi(bwd_hi, bwd_lo)),
        ky_hi=ky_hi,
        ky_lo=ky_lo,
        plane=np.stack([to_a, to_b, from_a, from_b]).reshape(4 * half * half, LANES),
    )
    places, at = {}, 0
    for name, part in parts.items():
        places[name] = (at, at + part.shape[0])
        at += part.shape[0]
    return np.concatenate([np.asarray(p, np.float32) for p in parts.values()], axis=0), places


class Tables:
    def __init__(self, ref, places):
        self.ref, self.places = ref, places

    def __getitem__(self, name):
        first, last = self.places[name]
        return self.ref[first:last]

    def row(self, name, i):
        first = self.places[name][0] + i
        return self.ref[first : first + 1]

    def block(self, name, i, n):
        first = self.places[name][0] + i * n
        return self.ref[first : first + n]

    def wide(self, name):
        both_halves = self[name].astype(BF16)
        n = both_halves.shape[0] // 2
        return jnp.concatenate([both_halves[:n], both_halves[n:]], axis=1)


def lower_half(shape):
    return lax.broadcasted_iota(jnp.int32, shape, len(shape) - 1) < HALF


def swap_halves(v):
    return pltpu.roll(v, HALF, axis=v.ndim - 1)


def hi_lo(v):
    high = v.astype(BF16)
    return high, (v - high.astype(F32)).astype(BF16)


def y_transform(v, tab):
    high, low = hi_lo(v)
    table = tab["ky_hi"].astype(BF16)
    return jnp.dot(
        jnp.concatenate([high, low], axis=1), jnp.concatenate([table, table], axis=0), preferred_element_type=F32
    ) + jnp.dot(high, tab["ky_lo"].astype(BF16), preferred_element_type=F32)


def x_transform(table, v):
    high, low = hi_lo(v)
    return jnp.dot(table, jnp.concatenate([high, low, high, jnp.zeros_like(high)], axis=0), preferred_element_type=F32)


def mix_rows(v, tab, first):
    swapped = swap_halves(v)
    half = v.shape[0]
    out = jnp.zeros_like(v)
    for r in range(half):
        a = tab.block("plane", first * half + r, half)
        b = tab.block("plane", (first + 1) * half + r, half)
        out = out + a * v[r : r + 1] + b * swapped[r : r + 1]
    return out


def gather(plane, mapping):
    half = plane.shape[0]
    bits = int(math.log2(half))
    ybits = int(math.log2(NY))
    row = (mapping >> ybits) & (half - 1)
    lane = ((mapping >> (ybits + bits)) << ybits) | (mapping & (NY - 1))
    out = jnp.zeros_like(plane)
    for r in range(half):
        source = jnp.broadcast_to(plane[r : r + 1], plane.shape)
        out = jnp.where(row == r, jnp.take_along_axis(source, lane, axis=1), out)
    return out


def position():
    is_fine = lax.axis_index("grp") == 0
    even = lax.rem(lax.axis_index("mesh"), 2) == 0
    return is_fine, even


def row_sign(is_fine, shape):
    odd = lax.rem(lax.broadcasted_iota(jnp.int32, shape, 0), 2) == 1
    return jnp.where(jnp.logical_and(odd, is_fine), -1.0, 1.0).astype(F32)


def pack_trace(full):
    n = full.shape[0] // 2
    return jnp.where(lower_half((n, LANES)), full[:n], full[n:])


def unpack_trace(packed):
    swapped = swap_halves(packed)
    low = lower_half(packed.shape)
    return jnp.concatenate([jnp.where(low, packed, swapped), jnp.where(low, swapped, packed)], axis=0)


def send_traces(u, even, to_even, to_odd):
    other = swap_halves(u)
    low = lower_half(u.shape)
    evens = jnp.where(low, u, other)
    odds = jnp.where(low, other, u)
    sign = jnp.where(even, 1.0, -1.0).astype(F32)
    to_even[...] = pack_trace(evens - sign * odds)
    to_odd[...] = pack_trace(evens + sign * odds)


def ghost_low_high(from_even, from_odd, even):
    a, b = unpack_trace(from_even[...]), unpack_trace(from_odd[...])
    return jnp.where(even, b, a), jnp.where(even, a, b)


def send_plane(y, tab, plane_out):
    plane_out[...] = mix_rows(y_transform(y, tab), tab, 2)


def x_ghost_tiles(ghost, is_fine):
    swapped = swap_halves(ghost)
    west = jnp.concatenate([swapped, ghost], axis=0)
    east = jnp.concatenate([ghost, swapped], axis=0)
    zero = jnp.zeros_like(west)
    return jnp.where(is_fine, zero, west), jnp.where(is_fine, east, zero)


def east_west(centre, before, after, low):
    east = swap_halves(jnp.where(low, after, centre))
    west = swap_halves(jnp.where(low, centre, before))
    return east, west


def north_south(centre):
    y = lax.broadcasted_iota(jnp.int32, centre.shape, 1) & (NY - 1)
    north = jnp.where(y == NY - 1, 0.0, pltpu.roll(centre, LANES - 1, axis=1))
    south = jnp.where(y == 0, 0.0, pltpu.roll(centre, 1, axis=1))
    return north, south


def strided(first, count, stride):
    return pl.ds(first, count, stride=stride)


def tile_lanes(t):
    return pl.ds(pl.multiple_of(t * LANES, LANES), LANES)


def pack_planes(state, planes, half, is_fine):
    low = lower_half((half, LANES))
    for f in range(FIELDS):
        first = state[f, :, 0:LANES]
        last = state[f, :, (TILES - 1) * LANES : TILES * LANES]
        fine = jnp.where(low, swap_halves(last[:half]), last[half:])
        coarse = jnp.where(low, first[:half], swap_halves(first[half:]))
        planes[f * half : (f + 1) * half] = jnp.where(is_fine, fine, coarse)


def pack_layers(value, f, t, height, even, to_even, to_odd):
    for k in range(2):
        bottom = value[k : k + 1]
        top = value[height - 2 + k : height - 1 + k]
        row = pl.ds((2 * f + k) * TILES + t, 1)
        to_even[row] = jnp.where(even, top, bottom)
        to_odd[row] = jnp.where(even, bottom, top)


def pack_kernel(height, state, to_even, to_odd, planes):
    is_fine, even = position()
    pack_planes(state, planes, height // 2, is_fine)

    def tile(t, _):
        for f in range(FIELDS):
            pack_layers(state[f, :, tile_lanes(t)], f, t, height, even, to_even, to_odd)
        return 0

    lax.fori_loop(0, TILES, tile, 0, unroll=UNROLL)


def z_mix(src, dst, tab, half, inverse):
    def chunk(r, _):
        rows = pl.ds(pl.multiple_of(r * 8, 8), 8)
        parts = [src[j, rows] for j in range(half)]
        for i in range(half):
            total = None
            for j in range(half):
                k = j * half + i if inverse else i * half + j
                term = tab.row("coef", k) * parts[j]
                total = term if total is None else total + term
            dst[i, rows] = total
        return 0

    lax.fori_loop(0, NX // 8, chunk, 0, unroll=8)


def base_kernel(height, places, current, burn, table, pad_a, pad_b, spectrum, trace, facet, source, folded, mixed):
    tab = Tables(table, places)
    is_fine, _ = position()
    half = height // 2
    tile_low = lower_half((height, LANES))
    z = lax.broadcasted_iota(jnp.int32, (height, LANES), 0)

    def tile(t, _):
        lanes = tile_lanes(t)
        row = pl.ds(pl.multiple_of((t + 1) * ROWS + ZERO_ROW, 8), height)
        u, v, w, fuel, oxygen = [current[f, :, lanes] for f in range(FIELDS)]
        pad_a[0, row], pad_a[1, row], pad_a[2, row] = u, v, w
        pad_b[0, row], pad_b[1, row] = fuel, oxygen
        before = jnp.where(t == 0, 0.0, current[0, :, tile_lanes(jnp.maximum(t - 1, 0))])
        after = jnp.where(t == TILES - 1, 0.0, current[0, :, tile_lanes(jnp.minimum(t + 1, TILES - 1))])
        east, west = east_west(u, before, after, tile_low)
        north, south = north_south(v)
        above = jnp.where(z == height - 1, 0.0, pltpu.roll(w, height - 1, axis=0))
        below = jnp.where(z == 0, 0.0, pltpu.roll(w, 1, axis=0))
        reaction = burn[:, lanes] * fuel * oxygen
        divergence = (east - west) + (north - south) + (above - below)
        source[pl.ds(pl.multiple_of(t * height, height), height)] = EXPANSION * reaction - 0.5 * divergence
        return 0

    lax.fori_loop(0, TILES, tile, 0, unroll=UNROLL)

    low = lower_half((TILES, LANES))
    for q in range(half):
        a = source[strided(q, TILES, height)]
        b = source[strided(height - 1 - q, TILES, height)]
        total, delta = a + b, a - b
        folded[q, 0:TILES] = jnp.where(low, total, swap_halves(delta))
        folded[q, TILES : 2 * TILES] = jnp.where(low, swap_halves(total), delta)

    z_mix(folded, mixed, tab, half, False)
    wide = jnp.concatenate([mixed[p] for p in range(half)], axis=1)
    wide = x_transform(tab.wide("fwd"), wide)
    tall = jnp.concatenate([wide[:, p * LANES : (p + 1) * LANES] for p in range(half)], axis=0)
    mixed[...] = y_transform(tall, tab).reshape(half, NX, LANES)

    column = tab["col_x"] * row_sign(is_fine, (NX, LANES))
    u0 = jnp.zeros((NX, LANES), F32)
    for p in range(half):
        solved = mixed[p] * tab.block("inv", p, NX)
        spectrum[p] = solved
        u0 = u0 + tab.row("edge", p) * solved
        facet[p : p + 1] = jnp.sum(column * solved, axis=0, keepdims=True)
    trace[...] = u0


def ghost_modes(plane, mapping, tab):
    return y_transform(mix_rows(gather(plane, mapping), tab, 0), tab)


def respond(layers, side, trace, facet, cross_rows, tab, half, is_fine):
    sign = row_sign(is_fine, (NX, LANES))
    signed = sign * layers
    cross_sum = jnp.zeros((NX, LANES), F32)
    for p in range(half):
        cross = tab.block("cross", p, NX)
        cross_sum = cross_sum + cross * side[p : p + 1]
        cross_rows[p : p + 1] = jnp.sum(cross * signed, axis=0, keepdims=True)
    u = trace[...] + tab["diag_z"] * layers + sign * cross_sum
    return u, facet[...] + tab["diag_x"] * side + cross_rows[...]


def add_kernel(height, places, from_even, from_odd, planes, mapping, trace, facet, table, *outs):
    layers_out, side_out, trace_out, facet_out, to_even, to_odd, plane_out, cross_rows = outs
    tab = Tables(table, places)
    is_fine, even = position()
    half = height // 2
    first = slice(2 * 2 * TILES, (2 * 2 + 1) * TILES)
    second = slice((2 * 2 + 1) * TILES, (2 * 2 + 2) * TILES)
    below = jnp.where(even, from_odd[second], from_even[second])
    above = jnp.where(even, from_even[first], from_odd[first])
    low = lower_half((TILES, LANES))
    pair = jnp.concatenate(
        [jnp.where(low, below, swap_halves(above)), jnp.where(low, swap_halves(below), above)], axis=0
    )
    pair = y_transform(x_transform(tab.wide("fwd"), pair), tab)
    other = swap_halves(pair)
    layers = 0.5 * jnp.where(lower_half((NX, LANES)), pair - other, pair + other)
    side = jnp.where(is_fine, -0.5, 0.5).astype(F32) * ghost_modes(planes[0:half], mapping[...], tab)
    u, y = respond(layers, side, trace, facet, cross_rows, tab, half, is_fine)
    layers_out[...] = layers
    side_out[...] = side
    trace_out[...] = u
    facet_out[...] = y
    send_traces(u, even, to_even, to_odd)
    send_plane(y, tab, plane_out)


def step_kernel(height, places, last, *refs):
    from_even, from_odd, plane_in, mapping, trace, facet, table, *outs = refs
    cross_rows = outs.pop()
    tab = Tables(table, places)
    to_even, to_odd, plane_out = outs[-3:]
    is_fine, even = position()
    half = height // 2
    low_ghost, high_ghost = ghost_low_high(from_even, from_odd, even)
    layers = jnp.where(lower_half((NX, LANES)), low_ghost + high_ghost, low_ghost - high_ghost)
    side = ghost_modes(plane_in[...], mapping[...], tab)
    if last:
        outs[0][...] = layers
        outs[1][...] = side
    u, y = respond(layers, side, trace, facet, cross_rows, tab, half, is_fine)
    send_traces(u, even, to_even, to_odd)
    send_plane(y, tab, plane_out)


def tend_kernel(height, fields, second, *refs):
    refs = list(refs)
    pad_in, current, burn, from_even, from_odd, planes, mapping = refs[:7]
    initial = refs[7] if second else None
    predicted, pad = refs[-2:]
    is_fine, even = position()
    half = height // 2
    tile_low = lower_half((height, LANES))
    tiled = pad.reshape(len(fields), TILES + 2, ROWS, LANES)
    for i, f in enumerate(fields):
        ghost = gather(planes[f * half : (f + 1) * half], mapping[...])
        west, east = x_ghost_tiles(ghost, is_fine)
        pad[i, ZERO_ROW : ZERO_ROW + height] = west
        last = (TILES + 1) * ROWS + ZERO_ROW
        pad[i, last : last + height] = east
        for k in range(2):
            rows = slice((2 * f + k) * TILES, (2 * f + k + 1) * TILES)
            below = jnp.where(even, from_odd[rows], from_even[rows])
            above = jnp.where(even, from_even[rows], from_odd[rows])
            pad[i, strided(ROWS + ZERO_ROW - 2 + k, TILES, ROWS)] = below
            pad[i, strided(ROWS + ZERO_ROW + height + k, TILES, ROWS)] = above

    def tile(t, _):
        lanes = tile_lanes(t)

        def at(i, dz=0, dt=0):
            return tiled[i, t + 1 + dt, ZERO_ROW + dz : ZERO_ROW + dz + height]

        cu = current[0, :, lanes] * (-0.5 * COURANT)
        cv = current[1, :, lanes] * (-0.5 * COURANT)
        cw = current[2, :, lanes] * (-COURANT / 12.0)
        if 3 in fields:
            reaction = burn[:, lanes] * current[3, :, lanes] * current[4, :, lanes]
        for i, f in enumerate(fields):
            centre = at(i)
            east, west = east_west(centre, at(i, 0, -1), at(i, 0, 1), tile_low)
            north, south = north_south(centre)
            above, below = at(i, 1), at(i, -1)
            above_two, below_two = at(i, 2), at(i, -2)
            dz = above - below
            change = cu * (east - west) + cv * (north - south) + cw * (8.0 * dz - (above_two - below_two))
            change = change + DIFFUSION * ((east + west) + (north + south) + (above + below) - 6.0 * centre)
            if f == 3:
                change = change - reaction
            if f == 4:
                change = change - STOICHIOMETRY * reaction
            if second:
                predicted[i, :, lanes] = 0.5 * (initial[f, :, lanes] + centre + change)
            else:
                predicted[i, :, lanes] = centre + change
        return 0

    lax.fori_loop(0, TILES, tile, 0, unroll=UNROLL)


def unfold(v):
    low = lower_half((TILES, LANES))
    top, bottom = v[:TILES], v[TILES:]
    return jnp.where(low, top, swap_halves(bottom)), jnp.where(low, swap_halves(top), bottom)


def inverse_kernel(height, places, spectrum, layers_a, side_a, layers_b, side_b, table, pad, tall, mixed, unmixed):
    tab = Tables(table, places)
    is_fine, _ = position()
    half = height // 2
    column = tab["col_x"] * row_sign(is_fine, (NX, LANES))
    layers = layers_a[...] + layers_b[...]
    side = side_a[...] + side_b[...]
    for p in range(half):
        push = tab.row("edge", p) * layers + column * side[p : p + 1]
        tall[p * NX : (p + 1) * NX] = spectrum[p] + push * tab.block("inv", p, NX)
    cells = y_transform(tall[...], tab)
    wide = jnp.concatenate([cells[p * NX : (p + 1) * NX] for p in range(half)], axis=1)
    wide = x_transform(tab.wide("bwd"), wide)
    for p in range(half):
        mixed[p] = wide[:, p * LANES : (p + 1) * LANES]
    z_mix(mixed, unmixed, tab, half, True)
    first = ROWS + ZERO_ROW
    for q in range(half):
        evens, odds = unfold(unmixed[q])
        pad[strided(first + q, TILES, ROWS)] = evens + odds
        pad[strided(first + height - 1 - q, TILES, ROWS)] = evens - odds


def correct_kernel(height, places, final, *refs):
    refs = list(refs)
    from_even, from_odd, plane_in, mapping, pad_in, flow, scalars, table = refs[:8]
    pad = refs[-1]
    state = refs[8]
    is_fine, even = position()
    half = height // 2
    tab = Tables(table, places)
    low_ghost, high_ghost = ghost_low_high(from_even, from_odd, even)
    pair = jnp.where(lower_half((NX, LANES)), low_ghost, high_ghost)
    below, above = unfold(x_transform(tab.wide("bwd"), y_transform(pair, tab)))
    first = ROWS + ZERO_ROW
    pad[strided(first - 1, TILES, ROWS)] = below
    pad[strided(first + height, TILES, ROWS)] = above
    west, east = x_ghost_tiles(gather(plane_in[...], mapping[...]), is_fine)
    pad[ZERO_ROW : ZERO_ROW + height] = west
    last = (TILES + 1) * ROWS + ZERO_ROW
    pad[last : last + height] = east
    tile_low = lower_half((height, LANES))
    tiled = pad.reshape(TILES + 2, ROWS, LANES)

    def tile(t, _):
        lanes = tile_lanes(t)

        def at(dz=0, dt=0):
            return tiled[t + 1 + dt, ZERO_ROW + dz : ZERO_ROW + dz + height]

        centre = at()
        east, west = east_west(centre, at(0, -1), at(0, 1), tile_low)
        north, south = north_south(centre)
        slopes = (east - west, north - south, at(1) - at(-1))
        for f in range(FIELDS):
            if f < 3:
                value = flow[f, :, lanes] - 0.5 * slopes[f]
            else:
                value = scalars[f - 3, :, lanes]
            state[f, :, lanes] = value
            if not final:
                pack_layers(value, f, t, height, even, refs[9], refs[10])
        if final:
            refs[9][:, lanes] = centre
        return 0

    lax.fori_loop(0, TILES, tile, 0, unroll=UNROLL)
    if not final:
        pack_planes(state, refs[11], half, is_fine)


def swap_pairs(x, parity):
    count = lax.axis_size("mesh")
    route = []
    for low in range(parity, count - 1, 2):
        route += [(low, low + 1), (low + 1, low)]
    return lax.ppermute(x, "mesh", route)


def swap_partner(x):
    return lax.ppermute(x, "grp", [(0, 1), (1, 0)])


def exchange(to_even, to_odd, plane):
    return swap_pairs(to_even, 0), swap_pairs(to_odd, 1), swap_partner(plane)


def call(body, outs, scratch, name, mib, cost, aliases=None):
    return pl.pallas_call(
        body,
        out_shape=outs,
        scratch_shapes=[pltpu.VMEM(s, F32) for s in scratch],
        input_output_aliases=aliases or {},
        compiler_params=pltpu.CompilerParams(vmem_limit_bytes=mib * MIB),
        cost_estimate=pl.CostEstimate(flops=int(cost * MICROSECOND), bytes_accessed=0, transcendentals=0),
        name=name,
    )


def shards(state, burn_rate, face_map):
    height = state.shape[2]
    half = height // 2
    cells = NX * NY
    table, places = tables(height)
    table = jnp.asarray(table)
    shape = lambda *s: jax.ShapeDtypeStruct(s, F32)
    bind = functools.partial
    halo = shape(2 * FIELDS * TILES, LANES)
    packed = shape(NX // 2, LANES)
    plane = shape(half, LANES)
    planes_shape = shape(FIELDS * half, LANES)
    layer = shape(NX, LANES)
    spectral = shape(half, NX, LANES)
    padded = lambda *n: shape(*n, (TILES + 2) * ROWS, LANES)
    initial = state[0]
    burning = burn_rate[0]
    by_row = face_map[0, 0].reshape(height, NY)
    mapping = jnp.concatenate([by_row[:half], by_row[half:]], axis=1)
    groups = ((0, 1, 2), (3, 4))

    packets = call(bind(pack_kernel, height), (halo, halo, planes_shape), (), "pack", 8, 0.5)(initial)
    current = initial
    for section in range(SECTIONS):
        second = section > 0
        final = section == SECTIONS - 1
        halos = exchange(*packets)
        *pads, spectrum, trace, facet = call(
            bind(base_kernel, height, places),
            (padded(3), padded(2), spectral, layer, plane),
            ((TILES * height, LANES), (half, NX, LANES), (half, NX, LANES)),
            "base",
            16,
            3,
        )(current, burning, table)
        layers_a, side_a, trace, facet, *packets = call(
            bind(add_kernel, height, places),
            (layer, plane, layer, plane, packed, packed, plane),
            ((half, LANES),),
            "add",
            4,
            1,
        )(*halos, mapping, trace, facet, table)
        predicted = [
            call(
                bind(tend_kernel, height, fields, second),
                (shape(len(fields), height, cells), padded(len(fields))),
                (),
                "tend",
                16,
                2,
                {0: 1},
            )(pad, current, burning, *halos, mapping, *((initial,) if second else ()))[0]
            for fields, pad in zip(groups, pads)
        ]
        for sweep in range(ITERS - 1):
            last = sweep == ITERS - 2
            received = exchange(*packets)
            if sweep < len(predicted):
                received, predicted[sweep] = lax.optimization_barrier((received, predicted[sweep]))
            *kept, to_even, to_odd, plane_out = call(
                bind(step_kernel, height, places, last),
                ((layer, plane) if last else ()) + (packed, packed, plane),
                ((half, LANES),),
                "step",
                4,
                0.5,
            )(*received, mapping, trace, facet, table)
            packets = (to_even, to_odd, plane_out)
        received = exchange(*packets)
        pressure = call(
            bind(inverse_kernel, height, places),
            padded(),
            ((half * NX, LANES), (half, NX, LANES), (half, NX, LANES)),
            "inverse",
            8,
            2,
        )(spectrum, layers_a, side_a, *kept, table)
        current, *packets = call(
            bind(correct_kernel, height, places, final),
            (shape(FIELDS, height, cells),) + ((shape(height, cells),) if final else (halo, halo, planes_shape)) + (padded(),),
            (),
            "correct",
            16,
            2,
            {4: 2 if final else 4},
        )(*received, mapping, pressure, *predicted, table)
        packets = packets[:-1]
    return current[None], packets[0][None]


def solution(mesh):
    placed = (P("grp", None, "mesh", None), P("grp", "mesh", None), P("grp", "mesh", None))
    return jax.shard_map(
        shards,
        mesh=mesh,
        in_specs=placed,
        out_specs=(P("grp", None, "mesh", None), P("grp", "mesh", None)),
        check_vma=False,
    )
```
